32 devices in a mesh: patch: 16 (over z, x, core), tp: 2 (over y).
Axes of the slice: x: 2, y: 2, z: 4, core: 2. Of those that a mesh axis runs over, the one named last changes fastest.
Arguments:
- resid_corrupt: bfloat16 [512, 4096], P(None, 'tp'), may hold values from -6 to 6
- resid_clean: bfloat16 [2, 512, 4096], P(None, 'patch', 'tp'), may hold values from -6 to 6
- patch_level: int32 [16], P('patch'), may hold values from 0 to 1
- patch_mask: int32 [16, 128], P('patch'), may hold values 0 or 1
- norm_gain: bfloat16 [4096], P('tp'), may hold values from 0.099609375 to 1.8984375
- final_gain: bfloat16 [4096], P('tp'), may hold values from 0.099609375 to 1.8984375
- w_query: bfloat16 [4096, 4096], P('patch', 'tp'), may hold values from -1 to 1
- w_key: bfloat16 [4096, 1024], P('patch', 'tp'), may hold values from -1 to 1
- w_value: bfloat16 [4096, 1024], P('patch', 'tp'), may hold values from -0.09375 to 0.09375
- w_out: bfloat16 [4096, 4096], P('tp', 'patch'), may hold values from -0.09375 to 0.09375
- unembed: bfloat16 [128256, 4096], P(('patch', 'tp')), may hold values from -0.09375 to 0.09375
- scored_ids: int32 [256], replicated, may hold values from 0 to 128255
- base_logits: float32 [512, 256], P('tp'), may hold values from -6 to 6
Outputs:
- logit_shift: float32 [16, 512, 256], P('patch', 'tp')
The draws below stay inside these ranges and needn't reach their ends.
All inputs are finite; a program needn't handle non-finite values. No bound on the sum of `patch_mask` on one device may be relied on, other than what follows from the above.
Results may differ from the reference program's by a relative error of at most 0.01.
The reference program's roundings to bfloat16 on the way count: a program that leaves them out, or rounds other values in their place, can miss the bound.
Values may be sent and summed in bfloat16 or wider, within the bound.
No kernel may reach another device: no remote copies, remote signals or barrier semaphores. Data moves between devices by JAX's collectives and lax.ppermute only.
A program may use at most 192 MiB of HBM per device.

```python
import math
import jax
import jax.numpy as jnp
from jax import lax

D = 4096
H = 32
KVH = 8
HD = 128
VOCAB = 128256
SEQ = 128
PROMPTS = 4
NSITE = 2
SCORED = 256
TOKENS = 512
GROUPS = 16
N_TP = 2


def shared_keys(key):
    return jax.random.normal(jax.random.fold_in(key, 11), (D, KVH * HD), jnp.float32)


def draw_w_query(key, part):
    own = jax.random.normal(jax.random.fold_in(key, 12), (D, H * HD), jnp.float32)
    scaled = jnp.clip(own, -6.0, 6.0) / math.sqrt(D)
    return jnp.clip(scaled, -1.0, 1.0).astype(jnp.bfloat16)


def draw_w_key(key, part):
    shared = shared_keys(key)
    scaled = jnp.clip(shared, -6.0, 6.0) / math.sqrt(D)
    return jnp.clip(scaled, -1.0, 1.0).astype(jnp.bfloat16)


def set_ends(values, own_key, smallest, top_value):
    place = [jax.random.randint(jax.random.fold_in(own_key, axis), (), 0, length) for axis, length in enumerate(values.shape)]
    widest = values.shape.index(max(values.shape))
    next_to = place[:widest] + [(place[widest] + 1) % values.shape[widest]] + place[widest + 1:]
    return values.at[tuple(place)].set(smallest).at[tuple(next_to)].set(top_value)


def block_scale(stream_key, extent, split, smallest, top_value):
    def one(dim, parts):
        steps = jax.random.uniform(jax.random.fold_in(jax.random.fold_in(stream_key, 6), dim), (parts,), jnp.float32, smallest / len(split), top_value / len(split))
        return jnp.repeat(jnp.exp(steps), extent[dim] // parts).reshape((-1,) + (1,) * (len(extent) - dim - 1))

    loudness = one(*split[0])
    for cut in split[1:]:
        loudness = loudness * one(*cut)
    return loudness


def centred(stream_key, extent, scale, limit, split=(), kind=jnp.bfloat16):
    entries = scale * jax.random.normal(stream_key, extent, jnp.float32)
    if split:
        entries = entries * block_scale(stream_key, extent, split, -0.22, 0.18)
    return jnp.clip(entries, -limit, limit).astype(kind)


def setup_inputs(seed: int = 0) -> dict:
    streams_of = jax.random.split(jax.random.key(seed), 14)
    resid_corrupt = centred(streams_of[0], (TOKENS, D), 1.0, 6.0, ((1, 2),))
    resid_clean = centred(streams_of[1], (NSITE, TOKENS, D), 1.0, 6.0, ((1, 16), (2, 2)))
    patch_level = set_ends(jax.random.randint(streams_of[2], (GROUPS,), 0, NSITE), jax.random.fold_in(streams_of[2], 1), 0, NSITE - 1).astype(jnp.int32)
    patch_mask = set_ends((jax.random.randint(streams_of[3], (GROUPS, SEQ), 0, 4) < 1).astype(jnp.int32), jax.random.fold_in(streams_of[3], 1), 0, 1)
    norm_gain = jnp.clip(1.0 + 0.18 * jax.random.normal(streams_of[4], (D,), jnp.float32), 0.099609375, 1.8984375).astype(jnp.bfloat16)
    final_gain = jnp.clip(1.0 + 0.18 * jax.random.normal(streams_of[5], (D,), jnp.float32), 0.099609375, 1.8984375).astype(jnp.bfloat16)
    w_query = draw_w_query(jax.random.fold_in(streams_of[13], 71), 0)
    w_key = draw_w_key(jax.random.fold_in(streams_of[13], 71), 0)
    w_value = centred(streams_of[8], (D, KVH * HD), D ** -0.5, 0.09375, ((0, 16), (1, 2)))
    w_out = centred(streams_of[9], (H * HD, D), (H * HD) ** -0.5, 0.09375, ((0, 2), (1, 16)))
    unembed = centred(streams_of[10], (VOCAB, D), D ** -0.5, 0.09375, ((0, 32),))
    scored_ids = set_ends(jax.random.randint(streams_of[11], (SCORED,), 0, VOCAB), jax.random.fold_in(streams_of[11], 1), 0, VOCAB - 1).astype(jnp.int32)
    base_logits = centred(streams_of[12], (TOKENS, SCORED), 1.0, 6.0, ((0, 2),), jnp.float32)
    return dict(resid_corrupt=resid_corrupt, resid_clean=resid_clean, patch_level=patch_level, patch_mask=patch_mask, norm_gain=norm_gain, final_gain=final_gain, w_query=w_query, w_key=w_key, w_value=w_value, w_out=w_out, unembed=unembed, scored_ids=scored_ids, base_logits=base_logits)


EPSILON = 1e-05
THETA = 500000.0

def rope_tables(length, head_dim):
    half = head_dim // 2
    freqs = THETA ** (-(jnp.arange(half, dtype=jnp.float32) * 2.0 / head_dim))
    angles = jnp.arange(length, dtype=jnp.float32)[:, None] * freqs[None, :]
    return (jnp.cos(angles)[:, None, :], jnp.sin(angles)[:, None, :])

def rotate(values, cosine, sine):
    half = values.shape[-1] // 2
    lower = values[..., :half]
    upper = values[..., half:]
    return jnp.concatenate([lower * cosine - upper * sine, upper * cosine + lower * sine], axis=-1)

def rms_scale(rows, gain):
    return rows * lax.rsqrt(lax.optimization_barrier(jnp.mean(rows * rows, axis=-1, keepdims=True)) + EPSILON) * gain

def one_group(level, mask_row, resid_corrupt, resid_clean, norm_gain, final_gain, w_query, w_key, w_value, w_out, score_rows, base_logits):
    row_mask = jnp.tile(mask_row, PROMPTS) == 1
    early = (row_mask & (level == 0))[:, None]
    layer_in = jnp.where(early, resid_clean[0], resid_corrupt)
    normed = rms_scale(layer_in.astype(jnp.float32), norm_gain.astype(jnp.float32)).astype(jnp.bfloat16)
    query_f = jnp.dot(normed, w_query, preferred_element_type=jnp.float32)
    key_f = jnp.dot(normed, w_key, preferred_element_type=jnp.float32)
    value_rows = jnp.dot(normed, w_value, preferred_element_type=jnp.float32).astype(jnp.bfloat16)
    cosine, sine = rope_tables(SEQ, HD)
    group = H // KVH
    queries = rotate(query_f.reshape(PROMPTS, SEQ, H, HD), cosine, sine).astype(jnp.bfloat16)
    queries = queries.reshape(PROMPTS, SEQ, KVH, group, HD)
    key_rows = rotate(key_f.reshape(PROMPTS, SEQ, KVH, HD), cosine, sine).astype(jnp.bfloat16)
    value_rows = value_rows.reshape(PROMPTS, SEQ, KVH, HD)
    scores = jnp.einsum('pqkgd,pskd->pkgqs', queries.astype(jnp.float32), key_rows.astype(jnp.float32)) * HD ** (-0.5)
    causal = jnp.arange(SEQ)[:, None] >= jnp.arange(SEQ)[None, :]
    scores = jnp.where(causal, scores, -1e+30)
    probs = jax.nn.softmax(scores, axis=-1).astype(jnp.bfloat16)
    attended = jnp.einsum('pkgqs,pskd->pqkgd', probs.astype(jnp.float32), value_rows.astype(jnp.float32))
    attended = attended.astype(jnp.bfloat16).reshape(TOKENS, H * HD)
    width = H * HD // N_TP
    head_out = jnp.zeros((TOKENS, D), jnp.float32)
    for index in range(N_TP):
        term = jnp.dot(attended[:, index * width:(index + 1) * width], w_out[index * width:(index + 1) * width], preferred_element_type=jnp.float32).astype(jnp.bfloat16)
        head_out = head_out + lax.optimization_barrier(term).astype(jnp.float32)
    middle = layer_in.astype(jnp.float32) + head_out
    late = (row_mask & (level == 1))[:, None]
    residual = jnp.where(late, resid_clean[1].astype(jnp.float32), middle)
    final_rows = rms_scale(residual, final_gain.astype(jnp.float32)).astype(jnp.bfloat16)
    logits = jnp.dot(final_rows, score_rows.T, preferred_element_type=jnp.float32)
    return logits - base_logits

def reference(resid_corrupt, resid_clean, patch_level, patch_mask, norm_gain, final_gain, w_query, w_key, w_value, w_out, unembed, scored_ids, base_logits):
    score_rows = jnp.take(unembed, scored_ids.astype(jnp.int32), axis=0)

    def step(pair):
        return one_group(pair[0], pair[1], resid_corrupt, resid_clean, norm_gain, final_gain, w_query, w_key, w_value, w_out, score_rows, base_logits)
    return lax.map(step, (patch_level, patch_mask))
```

```python
import jax
import jax.numpy as jnp
from jax import lax
from jax.experimental import pallas as pl
from jax.experimental.pallas import tpu as pltpu
from jax.sharding import PartitionSpec as P

D = 4096
HD = 128
SEQ = 128
PROMPTS = 4
HALF = HD // 2

EPSILON = 1e-05
THETA = 500000.0


def is_power(n):
    return n & (n - 1) == 0


def xor_pairs(n, flip):
    return [(i, i ^ flip) for i in range(n)]


def swap_tp(x):
    return lax.ppermute(x, "tp", [(0, 1), (1, 0)])


def over_tp(x):
    n = lax.axis_size("tp")
    if n == 2:
        first = lax.axis_index("tp") == 0
        other = swap_tp(x)
        return [jnp.where(first, x, other), jnp.where(first, other, x)]
    every = lax.all_gather(x, "tp", axis=0)
    return [every[i] for i in range(n)]


def exchange_tp(x):
    n = lax.axis_size("tp")
    if n == 2:
        me = lax.axis_index("tp")
        first = me == 0
        mine = lax.dynamic_index_in_dim(x, me, 0, keepdims=False)
        other = swap_tp(lax.dynamic_index_in_dim(x, 1 - me, 0, keepdims=False))
        return [jnp.where(first, mine, other), jnp.where(first, other, mine)]
    got = lax.all_to_all(x, "tp", 0, 0, tiled=False)
    return [got[i] for i in range(n)]


def rope_angles(first, count):
    index = (first + lax.iota(jnp.int32, count)).astype(jnp.float32)
    freqs = THETA ** (-(index * 2.0 / HD))
    return lax.iota(jnp.int32, SEQ).astype(jnp.float32)[:, None] * freqs[None, :]


def rotate(values, first):
    count = values.shape[1] // 2
    angles = rope_angles(first, count)
    cosine = jnp.tile(jnp.cos(angles), (values.shape[0] // SEQ, 1))
    sine = jnp.tile(jnp.sin(angles), (values.shape[0] // SEQ, 1))
    lower, upper = values[:, :count], values[:, count:]
    return jnp.concatenate([lower * cosine - upper * sine, upper * cosine + lower * sine], axis=1)


def attend_body(q_ref, k_ref, v_ref, m_ref, o_ref):
    heads = q_ref.shape[0]
    patched = m_ref[0] > 0.5

    def pick(ref, *lead):
        clean = ref[lead + (1, 0)].astype(jnp.float32)
        corrupt = ref[lead + (0, 0)].astype(jnp.float32)
        return jnp.where(patched, clean, corrupt).astype(jnp.bfloat16)

    keys = pick(k_ref)
    values = pick(v_ref)
    queries = jnp.concatenate([pick(q_ref, h) for h in range(heads)], axis=0)
    scores = lax.dot_general(
        queries, keys, (((1,), (1,)), ((), ())), preferred_element_type=jnp.float32
    ) * HD ** (-0.5)
    row = lax.broadcasted_iota(jnp.int32, scores.shape, 0) % SEQ
    col = lax.broadcasted_iota(jnp.int32, scores.shape, 1)
    scores = jnp.where(row >= col, scores, -1e30)
    top = jnp.max(scores, axis=1, keepdims=True)
    weights = jnp.exp(scores - top)
    probs = (weights / jnp.sum(weights, axis=1, keepdims=True)).astype(jnp.bfloat16)
    out = jnp.dot(probs, values, preferred_element_type=jnp.float32).astype(jnp.bfloat16)
    for h in range(heads):
        o_ref[0, :, h * HD : (h + 1) * HD] = out[h * SEQ : (h + 1) * SEQ]


def attend(q, k, v, masks):
    heads, _, prompts = q.shape[:3]
    groups = masks.shape[0]
    return pl.pallas_call(
        attend_body,
        grid=(prompts, groups),
        in_specs=[
            pl.BlockSpec((heads, 2, 1, SEQ, HD), lambda p, g: (0, 0, p, 0, 0)),
            pl.BlockSpec((2, 1, SEQ, HD), lambda p, g: (0, p, 0, 0)),
            pl.BlockSpec((2, 1, SEQ, HD), lambda p, g: (0, p, 0, 0)),
            pl.BlockSpec((1, SEQ, HD), lambda p, g: (g, 0, 0)),
        ],
        out_specs=pl.BlockSpec((1, SEQ, heads * HD), lambda p, g: (g, p, 0)),
        out_shape=jax.ShapeDtypeStruct((groups, prompts * SEQ, heads * HD), jnp.bfloat16),
        name="attend",
    )(q, k, v, masks)


def on_device(
    resid_corrupt,
    resid_clean,
    patch_level,
    patch_mask,
    norm_gain,
    final_gain,
    w_query,
    w_key,
    w_value,
    w_out,
    unembed,
    scored_ids,
    base_logits,
):
    n_p, n_t = lax.axis_size("patch"), lax.axis_size("tp")
    me_p, me_t = lax.axis_index("patch"), lax.axis_index("tp")
    tokens = resid_corrupt.shape[0]
    slices_t = n_p // n_t
    sub = D // (n_p * n_t)
    kv_here = w_key.shape[1] // HD
    spread = n_p // kv_here
    per_kv = w_query.shape[1] // w_key.shape[1]
    me_a, me_b = me_p // kv_here, me_p % kv_here
    bf16, f32 = jnp.bfloat16, jnp.float32

    depth = w_query.shape[0]
    cut = spread // per_kv
    q_cols = w_query.reshape(depth, kv_here, per_kv, 2, cut, HALF // cut)
    q_cols = q_cols.transpose(2, 4, 1, 0, 3, 5).reshape(n_p, depth, HD // cut)
    k_cols = w_key.reshape(depth, kv_here, 2, spread, HALF // spread)
    k_cols = k_cols.transpose(3, 1, 0, 2, 4).reshape(n_p, depth, HD // spread)
    v_cols = w_value.reshape(depth, kv_here, spread, HD // spread)
    v_cols = v_cols.transpose(2, 1, 0, 3).reshape(n_p, depth, HD // spread)
    send = jnp.concatenate([q_cols, k_cols, v_cols], axis=2)
    width_q, width_kv = HD // cut, HD // spread

    clean_halves = over_tp(resid_clean[0])
    rows_here = resid_clean.shape[1]
    late_parts = exchange_tp(
        resid_clean[1].reshape(rows_here, slices_t, n_t, sub).transpose(2, 0, 1, 3)
    )
    late_part = jnp.concatenate(late_parts, axis=1).reshape(1, rows_here, n_p * sub)
    clean_all = lax.all_gather(
        jnp.concatenate([jnp.stack(clean_halves), late_part], axis=0), "patch", axis=1, tiled=True
    )
    corrupt_halves = over_tp(resid_corrupt)
    gain_full = jnp.concatenate(over_tp(norm_gain)).astype(f32)
    final_full = jnp.concatenate(over_tp(final_gain)).astype(f32)

    out_block = w_out.reshape(w_out.shape[0], n_t, sub).transpose(1, 0, 2)
    out_rows = jnp.concatenate(exchange_tp(out_block), axis=0)
    clean_all, out_rows = lax.optimization_barrier((clean_all, out_rows))
    out_cols = lax.all_gather(out_rows, "patch", axis=1, tiled=True)

    weights = lax.all_to_all(send, "patch", 0, 0, tiled=True).reshape(D, send.shape[2])

    def project(halves):
        rows = jnp.concatenate(halves, axis=1).astype(f32)
        scale = lax.rsqrt(jnp.mean(rows * rows, axis=1, keepdims=True) + EPSILON)
        normed = (rows * scale * gain_full).astype(bf16)
        return jnp.dot(normed, weights, preferred_element_type=f32)

    projected = jnp.concatenate(
        [project(corrupt_halves), project([clean_all[i] for i in range(n_t)])], axis=0
    )
    piece = jnp.concatenate(
        [
            rotate(projected[:, :width_q], (me_a % cut) * (HALF // cut)),
            rotate(projected[:, width_q : width_q + width_kv], me_a * (HALF // spread)),
            projected[:, width_q + width_kv :],
        ],
        axis=1,
    ).astype(bf16)

    if is_power(spread) and spread <= 8:
        got = [piece] + [
            lax.ppermute(piece, "patch", xor_pairs(n_p, k * kv_here)) for k in range(1, spread)
        ]
        got = jnp.stack(got)
        pieces = jnp.stack(
            [lax.dynamic_index_in_dim(got, me_a ^ i, 0, keepdims=False) for i in range(spread)]
        )
    else:
        sets = [[a * kv_here + b for a in range(spread)] for b in range(kv_here)]
        pieces = lax.all_gather(piece, "patch", axis=0, axis_index_groups=sets)
    all_rows = piece.shape[0]
    q = pieces[:, :, :width_q].reshape(per_kv, cut, all_rows, 2, HALF // cut)
    q = q.transpose(0, 2, 3, 1, 4).reshape(per_kv, 2, PROMPTS, SEQ, HD)
    k = pieces[:, :, width_q : width_q + width_kv].reshape(spread, all_rows, 2, HALF // spread)
    k = k.transpose(1, 2, 0, 3).reshape(2, PROMPTS, SEQ, HD)
    v = pieces[:, :, width_q + width_kv :].transpose(1, 0, 2).reshape(2, PROMPTS, SEQ, HD)

    early_here = (patch_mask * (patch_level[0] == 0)).astype(f32)
    if is_power(kv_here):
        early = [early_here] + [
            lax.ppermute(early_here, "patch", xor_pairs(n_p, k)) for k in range(1, kv_here)
        ]
        early = jnp.concatenate(early, axis=0)
    masks = jnp.broadcast_to(early[:, :, None], (kv_here, SEQ, HD))
    attended = attend(q, k, v, masks)

    mine = [attended[0]] + [
        lax.ppermute(attended[j], "patch", xor_pairs(n_p, j)) for j in range(1, kv_here)
    ]

    def in_order(slots):
        stacked = jnp.stack(slots)
        return jnp.concatenate(
            [
                lax.dynamic_index_in_dim(stacked, me_b ^ j, 0, keepdims=False)
                for j in range(kv_here)
            ],
            axis=1,
        )

    by_slot = [over_tp(x) for x in mine]
    rows_t = w_out.shape[0]
    row_mask = jnp.tile(patch_mask[0], PROMPTS) == 1
    early_rows = jnp.tile(early_here[0], PROMPTS)[:, None] > 0.5
    late_rows = (row_mask & (patch_level[0] == 1))[:, None]

    def own_features(halves):
        parts = [
            lax.dynamic_index_in_dim(
                x.reshape(x.shape[0], slices_t, n_t, sub), me_t, 2, keepdims=False
            ).reshape(x.shape[0], slices_t * sub)
            for x in halves
        ]
        return jnp.concatenate(parts, axis=1)

    residual = jnp.where(
        early_rows,
        own_features([clean_all[i] for i in range(n_t)]),
        own_features(corrupt_halves),
    ).astype(f32)
    for i in range(n_t):
        term = jnp.dot(
            in_order([slot[i] for slot in by_slot]),
            out_cols[i * rows_t : (i + 1) * rows_t],
            preferred_element_type=f32,
        )
        residual = residual + term.astype(bf16).astype(f32)
    residual = jnp.where(late_rows, clean_all[n_t].astype(f32), residual)
    final_own = own_features([final_full.reshape(1, n_t, -1)[:, i] for i in range(n_t)])
    squares = jnp.sum(residual * residual, axis=1)
    final_block = (residual * final_own).astype(bf16)

    rows_dev = unembed.shape[0]
    local = scored_ids - lax.axis_index(("patch", "tp")) * rows_dev
    owned = (local >= 0) & (local < rows_dev)
    picked = jnp.where(
        owned[:, None], jnp.take(unembed, jnp.clip(local, 0, rows_dev - 1), axis=0), 0
    ).astype(bf16)
    block = lax.psum_scatter(picked, "patch", scatter_dimension=1, tiled=True)
    score = sum(
        x.astype(f32)
        for x in exchange_tp(block.reshape(block.shape[0], n_t, sub).transpose(1, 0, 2))
    ).astype(bf16)
    score_block = lax.all_gather(score, "patch", axis=1, tiled=True)

    logits = lax.dot_general(
        final_block, score_block, (((1,), (1,)), ((), ())), preferred_element_type=f32
    )
    share = tokens // n_t
    total = sum(exchange_tp(logits.reshape(n_t, share, -1)))
    square_sum = sum(exchange_tp(squares.reshape(n_t, share)))
    scaling = lax.rsqrt(square_sum / D + EPSILON)[:, None]
    return (total * scaling - base_logits)[None]


def solution(mesh):
    placed = (
        P(None, "tp"),
        P(None, "patch", "tp"),
        P("patch"),
        P("patch", None),
        P("tp"),
        P("tp"),
        P("patch", "tp"),
        P("patch", "tp"),
        P("patch", "tp"),
        P("tp", "patch"),
        P(("patch", "tp"), None),
        P(),
        P("tp", None),
    )
    return jax.shard_map(
        on_device, mesh=mesh, in_specs=placed, out_specs=P("patch", "tp", None), check_vma=False
    )
```

```python
import jax
import jax.numpy as jnp
from jax import lax
from jax.experimental import pallas as pl
from jax.experimental.pallas import tpu as pltpu
from jax.sharding import PartitionSpec as P


D = 4096
HD = 128
SEQ = 128
PROMPTS = 4
HALF = HD // 2

EPSILON = 1e-05
THETA = 500000.0


def is_power(n):
    return n & (n - 1) == 0


def xor_pairs(n, flip):
    return [(i, i ^ flip) for i in range(n)]


def swap_tp(x):
    return lax.ppermute(x, "tp", [(0, 1), (1, 0)])


def over_tp(x):
    n = lax.axis_size("tp")
    if n == 2:
        first = lax.axis_index("tp") == 0
        other = swap_tp(x)
        return [jnp.where(first, x, other), jnp.where(first, other, x)]
    every = lax.all_gather(x, "tp", axis=0)
    return [every[i] for i in range(n)]


def exchange_tp(x):
    n = lax.axis_size("tp")
    if n == 2:
        me = lax.axis_index("tp")
        first = me == 0
        mine = lax.dynamic_index_in_dim(x, me, 0, keepdims=False)
        other = swap_tp(lax.dynamic_index_in_dim(x, 1 - me, 0, keepdims=False))
        return [jnp.where(first, mine, other), jnp.where(first, other, mine)]
    got = lax.all_to_all(x, "tp", 0, 0, tiled=False)
    return [got[i] for i in range(n)]


def reduce_patch(x):
    n = lax.axis_size("patch")
    me = lax.axis_index("patch")
    flip = 1
    while flip < n:
        pairs = x.reshape((x.shape[0] // 2, 2) + x.shape[1:])
        bit = (me // flip) % 2
        send = lax.dynamic_index_in_dim(pairs, 1 - bit, 1, keepdims=False)
        keep = lax.dynamic_index_in_dim(pairs, bit, 1, keepdims=False)
        x = keep + lax.ppermute(send, "patch", xor_pairs(n, flip))
        flip *= 2
    return x[0]


def rope_angles(first, count):
    index = (first + lax.iota(jnp.int32, count)).astype(jnp.float32)
    freqs = THETA ** (-(index * 2.0 / HD))
    return lax.iota(jnp.int32, SEQ).astype(jnp.float32)[:, None] * freqs[None, :]


def rotate(values, first):
    count = values.shape[1] // 2
    angles = rope_angles(first, count)
    cosine = jnp.tile(jnp.cos(angles), (values.shape[0] // SEQ, 1))
    sine = jnp.tile(jnp.sin(angles), (values.shape[0] // SEQ, 1))
    lower, upper = values[:, :count], values[:, count:]
    return jnp.concatenate([lower * cosine - upper * sine, upper * cosine + lower * sine], axis=1)


def attend_body(q_ref, k_ref, v_ref, m_ref, o_ref):
    heads = q_ref.shape[0]
    patched = m_ref[0] > 0.5

    def pick(ref, *lead):
        clean = ref[lead + (1, 0)].astype(jnp.float32)
        corrupt = ref[lead + (0, 0)].astype(jnp.float32)
        return jnp.where(patched, clean, corrupt).astype(jnp.bfloat16)

    keys = pick(k_ref)
    values = pick(v_ref)
    queries = jnp.concatenate([pick(q_ref, h) for h in range(heads)], axis=0)
    scores = lax.dot_general(
        queries, keys, (((1,), (1,)), ((), ())), preferred_element_type=jnp.float32
    ) * HD ** (-0.5)
    row = lax.broadcasted_iota(jnp.int32, scores.shape, 0) % SEQ
    col = lax.broadcasted_iota(jnp.int32, scores.shape, 1)
    scores = jnp.where(row >= col, scores, -1e30)
    top = jnp.max(scores, axis=1, keepdims=True)
    weights = jnp.exp(scores - top)
    probs = (weights / jnp.sum(weights, axis=1, keepdims=True)).astype(jnp.bfloat16)
    out = jnp.dot(probs, values, preferred_element_type=jnp.float32).astype(jnp.bfloat16)
    for h in range(heads):
        o_ref[0, :, h * HD : (h + 1) * HD] = out[h * SEQ : (h + 1) * SEQ]


def attend(q, k, v, masks):
    heads, _, prompts = q.shape[:3]
    groups = masks.shape[0]
    return pl.pallas_call(
        attend_body,
        grid=(prompts, groups),
        in_specs=[
            pl.BlockSpec((heads, 2, 1, SEQ, HD), lambda p, g: (0, 0, p, 0, 0)),
            pl.BlockSpec((2, 1, SEQ, HD), lambda p, g: (0, p, 0, 0)),
            pl.BlockSpec((2, 1, SEQ, HD), lambda p, g: (0, p, 0, 0)),
            pl.BlockSpec((1, SEQ, HD), lambda p, g: (g, 0, 0)),
        ],
        out_specs=pl.BlockSpec((1, SEQ, heads * HD), lambda p, g: (g, p, 0)),
        out_shape=jax.ShapeDtypeStruct((groups, prompts * SEQ, heads * HD), jnp.bfloat16),
        name="attend",
    )(q, k, v, masks)


def splice_body(place_ref, corrupt_a, corrupt_b, clean_a, clean_b, late_ref, code_ref, o_ref):
    code = code_ref[...]
    code = jnp.concatenate([code, code], axis=1)
    corrupt = jnp.concatenate([corrupt_a[...], corrupt_b[...]], axis=1).astype(jnp.float32)
    clean = jnp.concatenate([clean_a[...], clean_b[...]], axis=1).astype(jnp.float32)
    rows = jnp.where(code == 1, clean, corrupt)
    rows = jnp.where(code == 2, late_ref[...].astype(jnp.float32), rows)
    o_ref[...] = rows.astype(jnp.bfloat16)


def splice(place, corrupt, clean, code, columns):
    tokens, sub = code.shape

    def lane(q, place):
        return 2 * q + place[0]

    return pl.pallas_call(
        splice_body,
        grid_spec=pltpu.PrefetchScalarGridSpec(
            num_scalar_prefetch=1,
            grid=(columns // (2 * sub),),
            in_specs=[
                pl.BlockSpec((tokens, sub), lambda i, s: (0, lane(2 * i, s))),
                pl.BlockSpec((tokens, sub), lambda i, s: (0, lane(2 * i + 1, s))),
                pl.BlockSpec((tokens, sub), lambda i, s: (0, lane(2 * i, s))),
                pl.BlockSpec((tokens, sub), lambda i, s: (0, lane(2 * i + 1, s))),
                pl.BlockSpec((tokens, 2 * sub), lambda i, s: (0, D // (2 * sub) + i)),
                pl.BlockSpec((tokens, sub), lambda i, s: (0, 0)),
            ],
            out_specs=pl.BlockSpec((tokens, 2 * sub), lambda i, s: (0, i)),
        ),
        out_shape=jax.ShapeDtypeStruct((tokens, columns), jnp.bfloat16),
        name="splice",
    )(place, corrupt, corrupt, clean, clean, clean, code)


def finish_body(place_ref, *refs):
    heads = [refs[:4], refs[4:8]]
    w_ref, base_ref, code_ref, gain_ref, score_ref = refs[8:13]
    o_ref, sum_ref = refs[13:]
    step = pl.program_id(0)
    rows = heads[0][0].shape[1]
    code = code_ref[...]
    code = jnp.concatenate([code, code], axis=1)
    base = base_ref[...].astype(jnp.float32)
    residual = base
    for half in range(2):
        term = None
        for slot in range(4):
            at = pl.multiple_of((half * 4 + (place_ref[1] ^ slot)) * rows, rows)
            part = jnp.dot(
                heads[half][slot][...], w_ref[pl.ds(at, rows), :], preferred_element_type=jnp.float32
            )
            term = part if term is None else term + part
        residual = residual + term.astype(jnp.bfloat16).astype(jnp.float32)
    residual = jnp.where(code == 2, base, residual)
    final = (residual * gain_ref[...].astype(jnp.float32)).astype(jnp.bfloat16)
    score = jnp.concatenate([score_ref[0], score_ref[1]], axis=1)
    logits = lax.dot_general(
        final, score, (((1,), (1,)), ((), ())), preferred_element_type=jnp.float32
    )
    squares = residual * residual
    squares = squares[:, : squares.shape[1] // 2] + squares[:, squares.shape[1] // 2 :]

    @pl.when(step == 0)
    def _():
        o_ref[...] = logits
        sum_ref[...] = squares

    @pl.when(step > 0)
    def _():
        o_ref[...] += logits
        sum_ref[...] += squares

    @pl.when(step == pl.num_programs(0) - 1)
    def _():
        total = jnp.sum(sum_ref[...], axis=1, keepdims=True)
        sum_ref[...] = jnp.broadcast_to(total, sum_ref.shape)


def finish(place, heads, weights, base, code, gain, score):
    tokens, block = heads[0].shape
    columns = weights.shape[1]
    scored, sub = score.shape[1:]

    whole = pl.BlockSpec((tokens, block), lambda i, s: (0, 0))
    return pl.pallas_call(
        finish_body,
        grid_spec=pltpu.PrefetchScalarGridSpec(
            num_scalar_prefetch=1,
            grid=(columns // (2 * sub),),
            in_specs=[whole] * 8
            + [
                pl.BlockSpec((weights.shape[0], 2 * sub), lambda i, s: (0, i)),
                pl.BlockSpec((tokens, 2 * sub), lambda i, s: (0, i)),
                pl.BlockSpec((tokens, sub), lambda i, s: (0, 0)),
                pl.BlockSpec((1, 2 * sub), lambda i, s: (0, i)),
                pl.BlockSpec((2, scored, sub), lambda i, s: (i, 0, 0)),
            ],
            out_specs=[
                pl.BlockSpec((tokens, scored), lambda i, s: (0, 0)),
                pl.BlockSpec((tokens, sub), lambda i, s: (0, 0)),
            ],
        ),
        out_shape=[
            jax.ShapeDtypeStruct((tokens, scored), jnp.float32),
            jax.ShapeDtypeStruct((tokens, sub), jnp.float32),
        ],
        name="finish",
    )(place, *heads, weights, base, code, gain, score)


def on_device(
    resid_corrupt,
    resid_clean,
    patch_level,
    patch_mask,
    norm_gain,
    final_gain,
    w_query,
    w_key,
    w_value,
    w_out,
    unembed,
    scored_ids,
    base_logits,
):
    n_p, n_t = lax.axis_size("patch"), lax.axis_size("tp")
    me_p, me_t = lax.axis_index("patch"), lax.axis_index("tp")
    tokens = resid_corrupt.shape[0]
    slices_t = n_p // n_t
    sub = D // (n_p * n_t)
    kv_here = w_key.shape[1] // HD
    spread = n_p // kv_here
    per_kv = w_query.shape[1] // w_key.shape[1]
    me_a, me_b = me_p // kv_here, me_p % kv_here
    bf16, f32 = jnp.bfloat16, jnp.float32
    fused = n_t == 2 and kv_here == 4 and sub == HD

    depth = w_query.shape[0]
    cut = spread // per_kv
    q_cols = w_query.reshape(depth, kv_here, per_kv, 2, cut, HALF // cut)
    q_cols = q_cols.transpose(2, 4, 1, 0, 3, 5).reshape(n_p, depth, HD // cut)
    k_cols = w_key.reshape(depth, kv_here, 2, spread, HALF // spread)
    k_cols = k_cols.transpose(3, 1, 0, 2, 4).reshape(n_p, depth, HD // spread)
    v_cols = w_value.reshape(depth, kv_here, spread, HD // spread)
    v_cols = v_cols.transpose(2, 1, 0, 3).reshape(n_p, depth, HD // spread)
    send = jnp.concatenate([q_cols, k_cols, v_cols], axis=2)
    width_q, width_kv = HD // cut, HD // spread
    weights = lax.all_to_all(send, "patch", 0, 0, tiled=True).reshape(D, send.shape[2])

    corrupt_full = jnp.concatenate(over_tp(resid_corrupt), axis=1)
    rows_here = resid_clean.shape[1]
    clean_rows = jnp.concatenate(over_tp(resid_clean[0]), axis=1)
    late_parts = exchange_tp(
        resid_clean[1].reshape(rows_here, slices_t, n_t, sub).transpose(2, 0, 1, 3)
    )
    late_rows_here = jnp.concatenate(late_parts, axis=1).reshape(rows_here, n_p * sub)
    both_sites = lax.all_gather(
        jnp.concatenate([clean_rows, late_rows_here], axis=1), "patch", axis=0, tiled=True
    )
    clean_full = both_sites[:, :D]
    gain_full = jnp.concatenate(over_tp(norm_gain)).astype(f32)
    final_full = jnp.concatenate(over_tp(final_gain)).astype(f32)

    out_block = w_out.reshape(w_out.shape[0], n_t, sub).transpose(1, 0, 2)
    if fused:
        swapped = swap_tp(lax.dynamic_index_in_dim(out_block, 1 - me_t, 0, keepdims=False))
        out_rows = jnp.concatenate(
            [lax.dynamic_index_in_dim(out_block, me_t, 0, keepdims=False), swapped], axis=0
        )
    else:
        out_rows = jnp.concatenate(exchange_tp(out_block), axis=0)
    out_cols = lax.all_gather(out_rows, "patch", axis=1, tiled=True)

    def project(rows):
        rows = rows.astype(f32)
        scale = lax.rsqrt(jnp.mean(rows * rows, axis=1, keepdims=True) + EPSILON)
        normed = (rows * scale * gain_full).astype(bf16)
        return jnp.dot(normed, weights, preferred_element_type=f32)

    projected = jnp.concatenate([project(corrupt_full), project(clean_full)], axis=0)
    piece = jnp.concatenate(
        [
            rotate(projected[:, :width_q], (me_a % cut) * (HALF // cut)),
            rotate(projected[:, width_q : width_q + width_kv], me_a * (HALF // spread)),
            projected[:, width_q + width_kv :],
        ],
        axis=1,
    ).astype(bf16)

    if is_power(spread) and spread <= 8:
        got = [piece] + [
            lax.ppermute(piece, "patch", xor_pairs(n_p, k * kv_here)) for k in range(1, spread)
        ]
        got = jnp.stack(got)
        pieces = jnp.stack(
            [lax.dynamic_index_in_dim(got, me_a ^ i, 0, keepdims=False) for i in range(spread)]
        )
    else:
        sets = [[a * kv_here + b for a in range(spread)] for b in range(kv_here)]
        pieces = lax.all_gather(piece, "patch", axis=0, axis_index_groups=sets)
    all_rows = piece.shape[0]
    q = pieces[:, :, :width_q].reshape(per_kv, cut, all_rows, 2, HALF // cut)
    q = q.transpose(0, 2, 3, 1, 4).reshape(per_kv, 2, PROMPTS, SEQ, HD)
    k = pieces[:, :, width_q : width_q + width_kv].reshape(spread, all_rows, 2, HALF // spread)
    k = k.transpose(1, 2, 0, 3).reshape(2, PROMPTS, SEQ, HD)
    v = pieces[:, :, width_q + width_kv :].transpose(1, 0, 2).reshape(2, PROMPTS, SEQ, HD)

    early_here = (patch_mask * (patch_level[0] == 0)).astype(f32)
    early = [early_here] + [
        lax.ppermute(early_here, "patch", xor_pairs(n_p, j)) for j in range(1, kv_here)
    ]
    early = jnp.concatenate(early, axis=0)
    masks = jnp.broadcast_to(early[:, :, None], (kv_here, SEQ, HD))
    attended = attend(q, k, v, masks)

    mine = [attended[0]] + [
        lax.ppermute(attended[j], "patch", xor_pairs(n_p, j)) for j in range(1, kv_here)
    ]

    rows_dev = unembed.shape[0]
    local = scored_ids - lax.axis_index(("patch", "tp")) * rows_dev
    owned = (local >= 0) & (local < rows_dev)
    picked = jnp.where(
        owned[:, None], jnp.take(unembed, jnp.clip(local, 0, rows_dev - 1), axis=0), 0
    ).astype(bf16)
    scored = picked.shape[0]
    block = reduce_patch(picked.reshape(scored, n_p, n_t * sub).transpose(1, 0, 2))
    by_sub = block.reshape(scored, n_t, sub).transpose(1, 0, 2)
    if fused:
        score = lax.dynamic_index_in_dim(by_sub, me_t, 0, keepdims=False) + swap_tp(
            lax.dynamic_index_in_dim(by_sub, 1 - me_t, 0, keepdims=False)
        )
    else:
        score = sum(exchange_tp(by_sub))
    score = lax.all_gather(score, "patch", axis=0, tiled=True).reshape(n_p, scored, sub)

    row_mask = jnp.tile(patch_mask[0], PROMPTS) == 1
    share = tokens // n_t
    final_own = lax.dynamic_index_in_dim(
        final_full.reshape(n_p, n_t, sub), me_t, 1, keepdims=False
    ).reshape(1, n_p * sub)
    if fused:
        heads = mine + [swap_tp(x) for x in mine]
        code = jnp.where(row_mask, 1 + patch_level[0], 0)
        code = jnp.broadcast_to(code[:, None], (tokens, sub))
        place = jnp.stack([me_t, me_b]).astype(jnp.int32)
        base = splice(place, corrupt_full, both_sites, code, n_p * sub)
        parts = finish(place, heads, out_cols, base, code, final_own, score)
        logits, squares = (x.reshape(n_t, share, -1) for x in parts)

        def halves(x):
            return (
                lax.dynamic_index_in_dim(x, me_t, 0, keepdims=False),
                lax.dynamic_index_in_dim(x, 1 - me_t, 0, keepdims=False),
            )

        logits_keep, logits_send = halves(logits)
        squares_keep, squares_send = halves(squares[:, :, 0])
        square_sum = squares_keep + swap_tp(squares_send)
        total = logits_keep + swap_tp(logits_send.astype(bf16)).astype(f32)
        scaling = lax.rsqrt(square_sum / D + EPSILON)[:, None]
        return (total * scaling - base_logits)[None]

    def in_order(slots):
        stacked = jnp.stack(slots)
        return jnp.concatenate(
            [
                lax.dynamic_index_in_dim(stacked, me_b ^ j, 0, keepdims=False)
                for j in range(kv_here)
            ],
            axis=1,
        )

    by_slot = [over_tp(x) for x in mine]
    rows_t = w_out.shape[0]
    early_rows = jnp.tile(early_here[0], PROMPTS)[:, None] > 0.5
    late_rows = (row_mask & (patch_level[0] == 1))[:, None]

    def own_features(x):
        own = lax.dynamic_index_in_dim(x.reshape(tokens, n_p, n_t, sub), me_t, 2, keepdims=False)
        return own.reshape(tokens, n_p * sub)

    residual = jnp.where(early_rows, own_features(clean_full), own_features(corrupt_full))
    residual = residual.astype(f32)
    for i in range(n_t):
        term = jnp.dot(
            in_order([slot[i] for slot in by_slot]),
            out_cols[i * rows_t : (i + 1) * rows_t],
            preferred_element_type=f32,
        )
        residual = residual + term.astype(bf16).astype(f32)
    residual = jnp.where(late_rows, both_sites[:, D:].astype(f32), residual)
    squares = jnp.sum(residual * residual, axis=1)
    final_block = (residual * final_own).astype(bf16).reshape(tokens, n_p, sub)
    logits = jnp.einsum("rpj,psj->rs", final_block, score, preferred_element_type=f32)
    total = sum(exchange_tp(logits.reshape(n_t, share, -1)))
    square_sum = sum(exchange_tp(squares.reshape(n_t, share)))
    scaling = lax.rsqrt(square_sum / D + EPSILON)[:, None]
    return (total * scaling - base_logits)[None]


def solution(mesh):
    placed = (
        P(None, "tp"),
        P(None, "patch", "tp"),
        P("patch"),
        P("patch", None),
        P("tp"),
        P("tp"),
        P("patch", "tp"),
        P("patch", "tp"),
        P("patch", "tp"),
        P("tp", "patch"),
        P(("patch", "tp"), None),
        P(),
        P("tp", None),
    )
    return jax.shard_map(
        on_device, mesh=mesh, in_specs=placed, out_specs=P("patch", "tp", None), check_vma=False
    )
```

```python
import jax
import jax.numpy as jnp
from jax import lax
from jax.experimental import pallas as pl
from jax.experimental.pallas import tpu as pltpu
from jax.sharding import PartitionSpec as P


D = 4096
HD = 128
SEQ = 128
PROMPTS = 4
HALF = HD // 2

EPSILON = 1e-05
THETA = 500000.0


def is_power(n):
    return n & (n - 1) == 0


def xor_pairs(n, flip):
    return [(i, i ^ flip) for i in range(n)]


def swap_tp(x):
    return lax.ppermute(x, "tp", [(0, 1), (1, 0)])


def over_tp(x):
    n = lax.axis_size("tp")
    if n == 2:
        first = lax.axis_index("tp") == 0
        other = swap_tp(x)
        return [jnp.where(first, x, other), jnp.where(first, other, x)]
    every = lax.all_gather(x, "tp", axis=0)
    return [every[i] for i in range(n)]


def exchange_tp(x):
    n = lax.axis_size("tp")
    if n == 2:
        me = lax.axis_index("tp")
        first = me == 0
        mine = lax.dynamic_index_in_dim(x, me, 0, keepdims=False)
        other = swap_tp(lax.dynamic_index_in_dim(x, 1 - me, 0, keepdims=False))
        return [jnp.where(first, mine, other), jnp.where(first, other, mine)]
    got = lax.all_to_all(x, "tp", 0, 0, tiled=False)
    return [got[i] for i in range(n)]


def reduce_patch(x):
    n = lax.axis_size("patch")
    me = lax.axis_index("patch")
    flip = 1
    while flip < n:
        pairs = x.reshape((x.shape[0] // 2, 2) + x.shape[1:])
        bit = (me // flip) % 2
        send = lax.dynamic_index_in_dim(pairs, 1 - bit, 1, keepdims=False)
        keep = lax.dynamic_index_in_dim(pairs, bit, 1, keepdims=False)
        x = keep + lax.ppermute(send, "patch", xor_pairs(n, flip))
        flip *= 2
    return x[0]


def gather_patch(x):
    n = lax.axis_size("patch")
    me = lax.axis_index("patch")
    got = x[None]
    flip = n // 2
    while flip:
        other = lax.ppermute(got, "patch", xor_pairs(n, flip))
        low = (me // flip) % 2 == 0
        got = jnp.stack([jnp.where(low, got, other), jnp.where(low, other, got)], axis=1)
        got = got.reshape((-1,) + x.shape)
        flip //= 2
    return got


def rope_angles(first, count):
    index = (first + lax.iota(jnp.int32, count)).astype(jnp.float32)
    freqs = THETA ** (-(index * 2.0 / HD))
    return lax.iota(jnp.int32, SEQ).astype(jnp.float32)[:, None] * freqs[None, :]


def rotate(values, first):
    count = values.shape[1] // 2
    angles = rope_angles(first, count)
    cosine = jnp.tile(jnp.cos(angles), (values.shape[0] // SEQ, 1))
    sine = jnp.tile(jnp.sin(angles), (values.shape[0] // SEQ, 1))
    lower, upper = values[:, :count], values[:, count:]
    return jnp.concatenate([lower * cosine - upper * sine, upper * cosine + lower * sine], axis=1)


def attend_body(q_ref, k_ref, v_ref, m_ref, o_ref):
    heads = q_ref.shape[0]
    patched = m_ref[0] > 0.5

    def pick(ref, *lead):
        clean = ref[lead + (1, 0)].astype(jnp.float32)
        corrupt = ref[lead + (0, 0)].astype(jnp.float32)
        return jnp.where(patched, clean, corrupt).astype(jnp.bfloat16)

    keys = pick(k_ref)
    values = pick(v_ref)
    queries = jnp.concatenate([pick(q_ref, h) for h in range(heads)], axis=0)
    scores = lax.dot_general(
        queries, keys, (((1,), (1,)), ((), ())), preferred_element_type=jnp.float32
    ) * HD ** (-0.5)
    row = lax.broadcasted_iota(jnp.int32, scores.shape, 0) % SEQ
    col = lax.broadcasted_iota(jnp.int32, scores.shape, 1)
    scores = jnp.where(row >= col, scores, -1e30)
    top = jnp.max(scores, axis=1, keepdims=True)
    weights = jnp.exp(scores - top)
    probs = (weights / jnp.sum(weights, axis=1, keepdims=True)).astype(jnp.bfloat16)
    out = jnp.dot(probs, values, preferred_element_type=jnp.float32).astype(jnp.bfloat16)
    for h in range(heads):
        o_ref[0, :, h * HD : (h + 1) * HD] = out[h * SEQ : (h + 1) * SEQ]


def attend(q, k, v, masks):
    heads, _, prompts = q.shape[:3]
    groups = masks.shape[0]
    return pl.pallas_call(
        attend_body,
        grid=(prompts, groups),
        in_specs=[
            pl.BlockSpec((heads, 2, 1, SEQ, HD), lambda p, g: (0, 0, p, 0, 0)),
            pl.BlockSpec((2, 1, SEQ, HD), lambda p, g: (0, p, 0, 0)),
            pl.BlockSpec((2, 1, SEQ, HD), lambda p, g: (0, p, 0, 0)),
            pl.BlockSpec((1, SEQ, HD), lambda p, g: (g, 0, 0)),
        ],
        out_specs=pl.BlockSpec((1, SEQ, heads * HD), lambda p, g: (g, p, 0)),
        out_shape=jax.ShapeDtypeStruct((groups, prompts * SEQ, heads * HD), jnp.bfloat16),
        name="attend",
    )(q, k, v, masks)


def splice_body(place_ref, corrupt_a, corrupt_b, clean_a, clean_b, code_ref, o_ref):
    code = code_ref[...]
    code = jnp.concatenate([code, code], axis=1)
    corrupt = jnp.concatenate([corrupt_a[...], corrupt_b[...]], axis=1).astype(jnp.float32)
    clean = jnp.concatenate([clean_a[...], clean_b[...]], axis=1).astype(jnp.float32)
    o_ref[...] = jnp.where(code == 1, clean, corrupt).astype(jnp.bfloat16)


def splice(place, corrupt, clean, code, columns):
    tokens, sub = code.shape

    def lane(q, place):
        return 2 * q + place[0]

    return pl.pallas_call(
        splice_body,
        grid_spec=pltpu.PrefetchScalarGridSpec(
            num_scalar_prefetch=1,
            grid=(columns // (2 * sub),),
            in_specs=[
                pl.BlockSpec((tokens, sub), lambda i, s: (0, lane(2 * i, s))),
                pl.BlockSpec((tokens, sub), lambda i, s: (0, lane(2 * i + 1, s))),
                pl.BlockSpec((tokens, sub), lambda i, s: (0, lane(2 * i, s))),
                pl.BlockSpec((tokens, sub), lambda i, s: (0, lane(2 * i + 1, s))),
                pl.BlockSpec((tokens, sub), lambda i, s: (0, 0)),
            ],
            out_specs=pl.BlockSpec((tokens, 2 * sub), lambda i, s: (0, i)),
        ),
        out_shape=jax.ShapeDtypeStruct((tokens, columns), jnp.bfloat16),
        name="splice",
    )(place, corrupt, corrupt, clean, clean, code)


def finish_body(place_ref, *refs):
    heads = [refs[:4], refs[4:8]]
    w_ref, base_ref, gain_ref, score_ref = refs[8:12]
    o_ref, sum_ref = refs[12:]
    step = pl.program_id(0)
    rows = heads[0][0].shape[1]
    residual = base_ref[...].astype(jnp.float32)
    for half in range(2):
        term = None
        for slot in range(4):
            at = pl.multiple_of((half * 4 + (place_ref[1] ^ slot)) * rows, rows)
            part = jnp.dot(
                heads[half][slot][...],
                jnp.concatenate([w_ref[0, pl.ds(at, rows), :], w_ref[1, pl.ds(at, rows), :]], axis=1),
                preferred_element_type=jnp.float32,
            )
            term = part if term is None else term + part
        residual = residual + term.astype(jnp.bfloat16).astype(jnp.float32)
    final = (residual * gain_ref[...].astype(jnp.float32)).astype(jnp.bfloat16)
    score = jnp.concatenate([score_ref[0], score_ref[1]], axis=1)
    logits = lax.dot_general(
        final, score, (((1,), (1,)), ((), ())), preferred_element_type=jnp.float32
    )
    squares = residual * residual
    squares = squares[:, : squares.shape[1] // 2] + squares[:, squares.shape[1] // 2 :]

    @pl.when(step == 0)
    def _():
        o_ref[...] = logits
        sum_ref[...] = squares

    @pl.when(step > 0)
    def _():
        o_ref[...] += logits
        sum_ref[...] += squares

    @pl.when(step == pl.num_programs(0) - 1)
    def _():
        total = jnp.sum(sum_ref[...], axis=1, keepdims=True)
        sum_ref[...] = jnp.broadcast_to(total, sum_ref.shape)


def finish(place, heads, weights, base, gain, score):
    tokens, block = heads[0].shape
    columns = base.shape[1]
    scored, sub = score.shape[1:]

    whole = pl.BlockSpec((tokens, block), lambda i, s: (0, 0))
    return pl.pallas_call(
        finish_body,
        grid_spec=pltpu.PrefetchScalarGridSpec(
            num_scalar_prefetch=1,
            grid=(columns // (2 * sub),),
            in_specs=[whole] * 8
            + [
                pl.BlockSpec((2, weights.shape[1], sub), lambda i, s: (i, 0, 0)),
                pl.BlockSpec((tokens, 2 * sub), lambda i, s: (0, i)),
                pl.BlockSpec((1, 2 * sub), lambda i, s: (0, i)),
                pl.BlockSpec((2, scored, sub), lambda i, s: (i, 0, 0)),
            ],
            out_specs=[
                pl.BlockSpec((tokens, scored), lambda i, s: (0, 0)),
                pl.BlockSpec((tokens, sub), lambda i, s: (0, 0)),
            ],
        ),
        out_shape=[
            jax.ShapeDtypeStruct((tokens, scored), jnp.float32),
            jax.ShapeDtypeStruct((tokens, sub), jnp.float32),
        ],
        name="finish",
    )(place, *heads, weights, base, gain, score)


def on_device(
    resid_corrupt,
    resid_clean,
    patch_level,
    patch_mask,
    norm_gain,
    final_gain,
    w_query,
    w_key,
    w_value,
    w_out,
    unembed,
    scored_ids,
    base_logits,
):
    n_p, n_t = lax.axis_size("patch"), lax.axis_size("tp")
    me_p, me_t = lax.axis_index("patch"), lax.axis_index("tp")
    tokens = resid_corrupt.shape[0]
    slices_t = n_p // n_t
    sub = D // (n_p * n_t)
    kv_here = w_key.shape[1] // HD
    spread = n_p // kv_here
    per_kv = w_query.shape[1] // w_key.shape[1]
    me_a, me_b = me_p // kv_here, me_p % kv_here
    bf16, f32 = jnp.bfloat16, jnp.float32
    fused = n_t == 2 and kv_here == 4 and sub == HD

    depth = w_query.shape[0]
    cut = spread // per_kv
    q_cols = w_query.reshape(depth, kv_here, per_kv, 2, cut, HALF // cut)
    q_cols = q_cols.transpose(2, 4, 1, 0, 3, 5).reshape(n_p, depth, HD // cut)
    k_cols = w_key.reshape(depth, kv_here, 2, spread, HALF // spread)
    k_cols = k_cols.transpose(3, 1, 0, 2, 4).reshape(n_p, depth, HD // spread)
    v_cols = w_value.reshape(depth, kv_here, spread, HD // spread)
    v_cols = v_cols.transpose(2, 1, 0, 3).reshape(n_p, depth, HD // spread)
    send = jnp.concatenate([q_cols, k_cols, v_cols], axis=2)
    width_q, width_kv = HD // cut, HD // spread
    weights = lax.all_to_all(send, "patch", 0, 0, tiled=True).reshape(D, send.shape[2])

    corrupt_full = jnp.concatenate(over_tp(resid_corrupt), axis=1)
    rows_here = resid_clean.shape[1]
    clean_rows = jnp.concatenate(over_tp(resid_clean[0]), axis=1)
    late_parts = exchange_tp(
        resid_clean[1].reshape(rows_here, slices_t, n_t, sub).transpose(2, 0, 1, 3)
    )
    late_rows_here = jnp.concatenate(late_parts, axis=1).reshape(rows_here, n_p * sub)
    clean_full = lax.all_gather(clean_rows, "patch", axis=0, tiled=True)
    gain_full = jnp.concatenate(over_tp(norm_gain)).astype(f32)
    final_full = jnp.concatenate(over_tp(final_gain)).astype(f32)

    out_block = w_out.reshape(w_out.shape[0], n_t, sub).transpose(1, 0, 2)
    if fused:
        swapped = swap_tp(lax.dynamic_index_in_dim(out_block, 1 - me_t, 0, keepdims=False))
        out_rows = jnp.concatenate(
            [lax.dynamic_index_in_dim(out_block, me_t, 0, keepdims=False), swapped], axis=0
        )
    else:
        out_rows = jnp.concatenate(exchange_tp(out_block), axis=0)
    if fused:
        out_cols = lax.all_gather(out_rows, "patch", axis=0, tiled=True)
        out_cols = out_cols.reshape((n_p,) + out_rows.shape)
    else:
        out_cols = lax.all_gather(out_rows, "patch", axis=1, tiled=True)

    def project(rows):
        rows = rows.astype(f32)
        scale = lax.rsqrt(jnp.mean(rows * rows, axis=1, keepdims=True) + EPSILON)
        normed = (rows * scale * gain_full).astype(bf16)
        return jnp.dot(normed, weights, preferred_element_type=f32)

    projected = jnp.concatenate([project(corrupt_full), project(clean_full)], axis=0)
    piece = jnp.concatenate(
        [
            rotate(projected[:, :width_q], (me_a % cut) * (HALF // cut)),
            rotate(projected[:, width_q : width_q + width_kv], me_a * (HALF // spread)),
            projected[:, width_q + width_kv :],
        ],
        axis=1,
    ).astype(bf16)

    if is_power(spread) and spread <= 8:
        got = [piece] + [
            lax.ppermute(piece, "patch", xor_pairs(n_p, k * kv_here)) for k in range(1, spread)
        ]
        got = jnp.stack(got)
        pieces = jnp.stack(
            [lax.dynamic_index_in_dim(got, me_a ^ i, 0, keepdims=False) for i in range(spread)]
        )
    else:
        sets = [[a * kv_here + b for a in range(spread)] for b in range(kv_here)]
        pieces = lax.all_gather(piece, "patch", axis=0, axis_index_groups=sets)
    all_rows = piece.shape[0]
    q = pieces[:, :, :width_q].reshape(per_kv, cut, all_rows, 2, HALF // cut)
    q = q.transpose(0, 2, 3, 1, 4).reshape(per_kv, 2, PROMPTS, SEQ, HD)
    k = pieces[:, :, width_q : width_q + width_kv].reshape(spread, all_rows, 2, HALF // spread)
    k = k.transpose(1, 2, 0, 3).reshape(2, PROMPTS, SEQ, HD)
    v = pieces[:, :, width_q + width_kv :].transpose(1, 0, 2).reshape(2, PROMPTS, SEQ, HD)

    early_here = (patch_mask * (patch_level[0] == 0)).astype(f32)
    early = [early_here] + [
        lax.ppermute(early_here, "patch", xor_pairs(n_p, j)) for j in range(1, kv_here)
    ]
    early = jnp.concatenate(early, axis=0)
    masks = jnp.broadcast_to(early[:, :, None], (kv_here, SEQ, HD))
    attended = attend(q, k, v, masks)

    mine = [attended[0]] + [
        lax.ppermute(attended[j], "patch", xor_pairs(n_p, j)) for j in range(1, kv_here)
    ]

    rows_dev = unembed.shape[0]
    local = scored_ids - lax.axis_index(("patch", "tp")) * rows_dev
    owned = (local >= 0) & (local < rows_dev)
    picked = jnp.where(
        owned[:, None], jnp.take(unembed, jnp.clip(local, 0, rows_dev - 1), axis=0), 0
    ).astype(bf16)
    scored = picked.shape[0]
    block = reduce_patch(picked.reshape(scored, n_p, n_t * sub).transpose(1, 0, 2))
    by_sub = block.reshape(scored, n_t, sub).transpose(1, 0, 2)
    if fused:
        score = lax.dynamic_index_in_dim(by_sub, me_t, 0, keepdims=False) + swap_tp(
            lax.dynamic_index_in_dim(by_sub, 1 - me_t, 0, keepdims=False)
        )
    else:
        score = sum(exchange_tp(by_sub))
    score = lax.all_gather(score, "patch", axis=0, tiled=True).reshape(n_p, scored, sub)

    row_mask = jnp.tile(patch_mask[0], PROMPTS) == 1
    share = tokens // n_t
    final_own = lax.dynamic_index_in_dim(
        final_full.reshape(n_p, n_t, sub), me_t, 1, keepdims=False
    ).reshape(1, n_p * sub)

    late_f = late_rows_here.astype(f32)
    late_final = (late_f * final_own).astype(bf16).reshape(rows_here, n_p, sub)
    late_logits = jnp.einsum("rpj,psj->rs", late_final, score, preferred_element_type=f32)
    late_squares = jnp.broadcast_to(
        jnp.sum(late_f * late_f, axis=1, keepdims=True), (rows_here, HD)
    )
    packed = jnp.concatenate([late_logits, late_squares], axis=1)
    packed = packed + swap_tp(packed) if n_t == 2 else lax.psum(packed, "tp")
    packed = gather_patch(packed).reshape(tokens, scored + HD)
    packed = lax.dynamic_slice_in_dim(packed, me_t * share, share, 0)
    late_total, late_sum = packed[:, :scored], packed[:, scored]
    is_late = row_mask & (patch_level[0] == 1)
    is_late = lax.dynamic_slice_in_dim(is_late, me_t * share, share, 0)

    def scored_shift(total, square_sum):
        total = jnp.where(is_late[:, None], late_total, total)
        scaling = lax.rsqrt(jnp.where(is_late, late_sum, square_sum) / D + EPSILON)
        return (total * scaling[:, None] - base_logits)[None]

    if fused:
        heads = mine + [swap_tp(x) for x in mine]
        code = jnp.where(row_mask, 1 + patch_level[0], 0)
        code = jnp.broadcast_to(code[:, None], (tokens, sub))
        place = jnp.stack([me_t, me_b]).astype(jnp.int32)
        base = splice(place, corrupt_full, clean_full, code, n_p * sub)
        parts = finish(place, heads, out_cols, base, final_own, score)
        logits, squares = (x.reshape(n_t, share, -1) for x in parts)

        def halves(x):
            return (
                lax.dynamic_index_in_dim(x, me_t, 0, keepdims=False),
                lax.dynamic_index_in_dim(x, 1 - me_t, 0, keepdims=False),
            )

        logits_keep, logits_send = halves(logits)
        squares_keep, squares_send = halves(squares[:, :, 0])
        square_sum = squares_keep + swap_tp(squares_send)
        total = logits_keep + swap_tp(logits_send.astype(bf16)).astype(f32)
        return scored_shift(total, square_sum)

    def in_order(slots):
        stacked = jnp.stack(slots)
        return jnp.concatenate(
            [
                lax.dynamic_index_in_dim(stacked, me_b ^ j, 0, keepdims=False)
                for j in range(kv_here)
            ],
            axis=1,
        )

    by_slot = [over_tp(x) for x in mine]
    rows_t = w_out.shape[0]
    early_rows = jnp.tile(early_here[0], PROMPTS)[:, None] > 0.5

    def own_features(x):
        own = lax.dynamic_index_in_dim(x.reshape(tokens, n_p, n_t, sub), me_t, 2, keepdims=False)
        return own.reshape(tokens, n_p * sub)

    residual = jnp.where(early_rows, own_features(clean_full), own_features(corrupt_full))
    residual = residual.astype(f32)
    for i in range(n_t):
        term = jnp.dot(
            in_order([slot[i] for slot in by_slot]),
            out_cols[i * rows_t : (i + 1) * rows_t],
            preferred_element_type=f32,
        )
        residual = residual + term.astype(bf16).astype(f32)
    squares = jnp.sum(residual * residual, axis=1)
    final_block = (residual * final_own).astype(bf16).reshape(tokens, n_p, sub)
    logits = jnp.einsum("rpj,psj->rs", final_block, score, preferred_element_type=f32)
    total = sum(exchange_tp(logits.reshape(n_t, share, -1)))
    square_sum = sum(exchange_tp(squares.reshape(n_t, share)))
    return scored_shift(total, square_sum)


def solution(mesh):
    placed = (
        P(None, "tp"),
        P(None, "patch", "tp"),
        P("patch"),
        P("patch", None),
        P("tp"),
        P("tp"),
        P("patch", "tp"),
        P("patch", "tp"),
        P("patch", "tp"),
        P("tp", "patch"),
        P(("patch", "tp"), None),
        P(),
        P("tp", None),
    )
    return jax.shard_map(
        on_device, mesh=mesh, in_specs=placed, out_specs=P("patch", "tp", None), check_vma=False
    )
```

```python
import jax
import jax.numpy as jnp
from jax import lax
from jax.experimental import pallas as pl
from jax.experimental.pallas import tpu as pltpu
from jax.sharding import PartitionSpec as P


D = 4096
HD = 128
SEQ = 128
PROMPTS = 4
HALF = HD // 2

EPSILON = 1e-05
THETA = 500000.0


def is_power(n):
    return n & (n - 1) == 0


def xor_pairs(n, flip):
    return [(i, i ^ flip) for i in range(n)]


def swap_tp(x):
    return lax.ppermute(x, "tp", [(0, 1), (1, 0)])


def over_tp(x):
    n = lax.axis_size("tp")
    if n == 2:
        first = lax.axis_index("tp") == 0
        other = swap_tp(x)
        return [jnp.where(first, x, other), jnp.where(first, other, x)]
    every = lax.all_gather(x, "tp", axis=0)
    return [every[i] for i in range(n)]


def exchange_tp(x):
    n = lax.axis_size("tp")
    if n == 2:
        me = lax.axis_index("tp")
        first = me == 0
        mine = lax.dynamic_index_in_dim(x, me, 0, keepdims=False)
        other = swap_tp(lax.dynamic_index_in_dim(x, 1 - me, 0, keepdims=False))
        return [jnp.where(first, mine, other), jnp.where(first, other, mine)]
    got = lax.all_to_all(x, "tp", 0, 0, tiled=False)
    return [got[i] for i in range(n)]


def reduce_patch(x):
    n = lax.axis_size("patch")
    me = lax.axis_index("patch")
    flip = 1
    while flip < n:
        pairs = x.reshape((x.shape[0] // 2, 2) + x.shape[1:])
        bit = (me // flip) % 2
        send = lax.dynamic_index_in_dim(pairs, 1 - bit, 1, keepdims=False)
        keep = lax.dynamic_index_in_dim(pairs, bit, 1, keepdims=False)
        x = keep + lax.ppermute(send, "patch", xor_pairs(n, flip))
        flip *= 2
    return x[0]


def gather_patch(x):
    n = lax.axis_size("patch")
    me = lax.axis_index("patch")
    got = x[None]
    flip = n // 2
    while flip:
        other = lax.ppermute(got, "patch", xor_pairs(n, flip))
        low = (me // flip) % 2 == 0
        got = jnp.stack([jnp.where(low, got, other), jnp.where(low, other, got)], axis=1)
        got = got.reshape((-1,) + x.shape)
        flip //= 2
    return got


def rope_angles(first, count):
    index = (first + lax.iota(jnp.int32, count)).astype(jnp.float32)
    freqs = THETA ** (-(index * 2.0 / HD))
    return lax.iota(jnp.int32, SEQ).astype(jnp.float32)[:, None] * freqs[None, :]


def rotate(values, first):
    count = values.shape[1] // 2
    angles = rope_angles(first, count)
    cosine = jnp.tile(jnp.cos(angles), (values.shape[0] // SEQ, 1))
    sine = jnp.tile(jnp.sin(angles), (values.shape[0] // SEQ, 1))
    lower, upper = values[:, :count], values[:, count:]
    return jnp.concatenate([lower * cosine - upper * sine, upper * cosine + lower * sine], axis=1)


def attend_body(q_ref, k_ref, v_ref, m_ref, o_ref):
    heads = q_ref.shape[0]
    patched = m_ref[0] > 0.5

    def pick(ref, *lead):
        clean = ref[lead + (1, 0)].astype(jnp.float32)
        corrupt = ref[lead + (0, 0)].astype(jnp.float32)
        return jnp.where(patched, clean, corrupt).astype(jnp.bfloat16)

    keys = pick(k_ref)
    values = pick(v_ref)
    queries = jnp.concatenate([pick(q_ref, h) for h in range(heads)], axis=0)
    scores = lax.dot_general(
        queries, keys, (((1,), (1,)), ((), ())), preferred_element_type=jnp.float32
    ) * HD ** (-0.5)
    row = lax.broadcasted_iota(jnp.int32, scores.shape, 0) % SEQ
    col = lax.broadcasted_iota(jnp.int32, scores.shape, 1)
    scores = jnp.where(row >= col, scores, -1e30)
    top = jnp.max(scores, axis=1, keepdims=True)
    weights = jnp.exp(scores - top)
    probs = (weights / jnp.sum(weights, axis=1, keepdims=True)).astype(jnp.bfloat16)
    out = jnp.dot(probs, values, preferred_element_type=jnp.float32).astype(jnp.bfloat16)
    for h in range(heads):
        o_ref[0, :, h * HD : (h + 1) * HD] = out[h * SEQ : (h + 1) * SEQ]


def attend(q, k, v, masks):
    heads, _, prompts = q.shape[:3]
    groups = masks.shape[0]
    return pl.pallas_call(
        attend_body,
        grid=(prompts, groups),
        in_specs=[
            pl.BlockSpec((heads, 2, 1, SEQ, HD), lambda p, g: (0, 0, p, 0, 0)),
            pl.BlockSpec((2, 1, SEQ, HD), lambda p, g: (0, p, 0, 0)),
            pl.BlockSpec((2, 1, SEQ, HD), lambda p, g: (0, p, 0, 0)),
            pl.BlockSpec((1, SEQ, HD), lambda p, g: (g, 0, 0)),
        ],
        out_specs=pl.BlockSpec((1, SEQ, heads * HD), lambda p, g: (g, p, 0)),
        out_shape=jax.ShapeDtypeStruct((groups, prompts * SEQ, heads * HD), jnp.bfloat16),
        name="attend",
    )(q, k, v, masks)


def splice_body(place_ref, corrupt_a, corrupt_b, clean_a, clean_b, code_ref, o_ref):
    code = code_ref[...]
    code = jnp.concatenate([code, code], axis=1)
    corrupt = jnp.concatenate([corrupt_a[...], corrupt_b[...]], axis=1).astype(jnp.float32)
    clean = jnp.concatenate([clean_a[...], clean_b[...]], axis=1).astype(jnp.float32)
    o_ref[...] = jnp.where(code == 1, clean, corrupt).astype(jnp.bfloat16)


def splice(place, corrupt, clean, code, columns):
    tokens, sub = code.shape

    def lane(q, place):
        return 2 * q + place[0]

    return pl.pallas_call(
        splice_body,
        grid_spec=pltpu.PrefetchScalarGridSpec(
            num_scalar_prefetch=1,
            grid=(columns // (2 * sub),),
            in_specs=[
                pl.BlockSpec((tokens, sub), lambda i, s: (0, lane(2 * i, s))),
                pl.BlockSpec((tokens, sub), lambda i, s: (0, lane(2 * i + 1, s))),
                pl.BlockSpec((tokens, sub), lambda i, s: (0, lane(2 * i, s))),
                pl.BlockSpec((tokens, sub), lambda i, s: (0, lane(2 * i + 1, s))),
                pl.BlockSpec((tokens, sub), lambda i, s: (0, 0)),
            ],
            out_specs=pl.BlockSpec((tokens, 2 * sub), lambda i, s: (0, i)),
        ),
        out_shape=jax.ShapeDtypeStruct((tokens, columns), jnp.bfloat16),
        name="splice",
    )(place, corrupt, corrupt, clean, clean, code)


def finish_body(place_ref, *refs):
    heads = [refs[:4], refs[4:8]]
    w_refs = [refs[8:12], refs[12:16]]
    base_ref, gain_ref, score_ref = refs[16:19]
    o_ref, sum_ref = refs[19:]
    step = pl.program_id(0)
    residual = base_ref[...].astype(jnp.float32)
    for half in range(2):
        term = None
        for slot in range(4):
            w_ref = w_refs[half][slot]
            part = jnp.dot(
                heads[half][slot][...],
                jnp.concatenate([w_ref[0], w_ref[1]], axis=1),
                preferred_element_type=jnp.float32,
            )
            term = part if term is None else term + part
        residual = residual + term.astype(jnp.bfloat16).astype(jnp.float32)
    final = (residual * gain_ref[...].astype(jnp.float32)).astype(jnp.bfloat16)
    score = jnp.concatenate([score_ref[0], score_ref[1]], axis=1)
    logits = lax.dot_general(
        final, score, (((1,), (1,)), ((), ())), preferred_element_type=jnp.float32
    )
    squares = residual * residual
    squares = squares[:, : squares.shape[1] // 2] + squares[:, squares.shape[1] // 2 :]

    @pl.when(step == 0)
    def _():
        o_ref[...] = logits
        sum_ref[...] = squares

    @pl.when(step > 0)
    def _():
        o_ref[...] += logits
        sum_ref[...] += squares

    @pl.when(step == pl.num_programs(0) - 1)
    def _():
        total = jnp.sum(sum_ref[...], axis=1, keepdims=True)
        sum_ref[...] = jnp.broadcast_to(total, sum_ref.shape)


def finish(place, heads, weights, base, gain, score):
    tokens, block = heads[0].shape
    columns = base.shape[1]
    scored, sub = score.shape[1:]

    whole = pl.BlockSpec((tokens, block), lambda i, s: (0, 0))

    def rows_of(half, slot):
        return pl.BlockSpec(
            (2, block, sub), lambda i, s: (i, half * 4 + (s[1] ^ slot), 0)
        )

    return pl.pallas_call(
        finish_body,
        grid_spec=pltpu.PrefetchScalarGridSpec(
            num_scalar_prefetch=1,
            grid=(columns // (2 * sub),),
            in_specs=[whole] * 8
            + [rows_of(half, slot) for half in range(2) for slot in range(4)]
            + [
                pl.BlockSpec((tokens, 2 * sub), lambda i, s: (0, i)),
                pl.BlockSpec((1, 2 * sub), lambda i, s: (0, i)),
                pl.BlockSpec((2, scored, sub), lambda i, s: (i, 0, 0)),
            ],
            out_specs=[
                pl.BlockSpec((tokens, scored), lambda i, s: (0, 0)),
                pl.BlockSpec((tokens, sub), lambda i, s: (0, 0)),
            ],
        ),
        out_shape=[
            jax.ShapeDtypeStruct((tokens, scored), jnp.float32),
            jax.ShapeDtypeStruct((tokens, sub), jnp.float32),
        ],
        name="finish",
    )(place, *heads, *[weights] * 8, base, gain, score)


def on_device(
    resid_corrupt,
    resid_clean,
    patch_level,
    patch_mask,
    norm_gain,
    final_gain,
    w_query,
    w_key,
    w_value,
    w_out,
    unembed,
    scored_ids,
    base_logits,
):
    n_p, n_t = lax.axis_size("patch"), lax.axis_size("tp")
    me_p, me_t = lax.axis_index("patch"), lax.axis_index("tp")
    tokens = resid_corrupt.shape[0]
    slices_t = n_p // n_t
    sub = D // (n_p * n_t)
    kv_here = w_key.shape[1] // HD
    spread = n_p // kv_here
    per_kv = w_query.shape[1] // w_key.shape[1]
    me_a, me_b = me_p // kv_here, me_p % kv_here
    bf16, f32 = jnp.bfloat16, jnp.float32
    fused = n_t == 2 and kv_here == 4 and sub == HD

    depth = w_query.shape[0]
    cut = spread // per_kv
    q_cols = w_query.reshape(depth, kv_here, per_kv, 2, cut, HALF // cut)
    q_cols = q_cols.transpose(2, 4, 1, 0, 3, 5).reshape(n_p, depth, HD // cut)
    k_cols = w_key.reshape(depth, kv_here, 2, spread, HALF // spread)
    k_cols = k_cols.transpose(3, 1, 0, 2, 4).reshape(n_p, depth, HD // spread)
    v_cols = w_value.reshape(depth, kv_here, spread, HD // spread)
    v_cols = v_cols.transpose(2, 1, 0, 3).reshape(n_p, depth, HD // spread)
    send = jnp.concatenate([q_cols, k_cols, v_cols], axis=2)
    width_q, width_kv = HD // cut, HD // spread
    weights = lax.all_to_all(send, "patch", 0, 0, tiled=True).reshape(D, send.shape[2])

    corrupt_full = jnp.concatenate(over_tp(resid_corrupt), axis=1)
    rows_here = resid_clean.shape[1]
    clean_rows = jnp.concatenate(over_tp(resid_clean[0]), axis=1)
    late_parts = exchange_tp(
        resid_clean[1].reshape(rows_here, slices_t, n_t, sub).transpose(2, 0, 1, 3)
    )
    late_rows_here = jnp.concatenate(late_parts, axis=1).reshape(rows_here, n_p * sub)
    clean_full = lax.all_gather(clean_rows, "patch", axis=0, tiled=True)
    gain_full = jnp.concatenate(over_tp(norm_gain)).astype(f32)
    final_full = jnp.concatenate(over_tp(final_gain)).astype(f32)

    out_block = w_out.reshape(w_out.shape[0], n_t, sub).transpose(1, 0, 2)
    if fused:
        swapped = swap_tp(lax.dynamic_index_in_dim(out_block, 1 - me_t, 0, keepdims=False))
        out_rows = jnp.concatenate(
            [lax.dynamic_index_in_dim(out_block, me_t, 0, keepdims=False), swapped], axis=0
        )
    else:
        out_rows = jnp.concatenate(exchange_tp(out_block), axis=0)
    if fused:
        out_cols = lax.all_gather(out_rows, "patch", axis=0, tiled=True)
        out_cols = out_cols.reshape((n_p,) + out_rows.shape)
    else:
        out_cols = lax.all_gather(out_rows, "patch", axis=1, tiled=True)

    def project(rows):
        rows = rows.astype(f32)
        scale = lax.rsqrt(jnp.mean(rows * rows, axis=1, keepdims=True) + EPSILON)
        normed = (rows * scale * gain_full).astype(bf16)
        return jnp.dot(normed, weights, preferred_element_type=f32)

    projected = jnp.concatenate([project(corrupt_full), project(clean_full)], axis=0)
    piece = jnp.concatenate(
        [
            rotate(projected[:, :width_q], (me_a % cut) * (HALF // cut)),
            rotate(projected[:, width_q : width_q + width_kv], me_a * (HALF // spread)),
            projected[:, width_q + width_kv :],
        ],
        axis=1,
    ).astype(bf16)

    if is_power(spread) and spread <= 8:
        got = [piece] + [
            lax.ppermute(piece, "patch", xor_pairs(n_p, k * kv_here)) for k in range(1, spread)
        ]
        got = jnp.stack(got)
        pieces = jnp.stack(
            [lax.dynamic_index_in_dim(got, me_a ^ i, 0, keepdims=False) for i in range(spread)]
        )
    else:
        sets = [[a * kv_here + b for a in range(spread)] for b in range(kv_here)]
        pieces = lax.all_gather(piece, "patch", axis=0, axis_index_groups=sets)
    all_rows = piece.shape[0]
    q = pieces[:, :, :width_q].reshape(per_kv, cut, all_rows, 2, HALF // cut)
    q = q.transpose(0, 2, 3, 1, 4).reshape(per_kv, 2, PROMPTS, SEQ, HD)
    k = pieces[:, :, width_q : width_q + width_kv].reshape(spread, all_rows, 2, HALF // spread)
    k = k.transpose(1, 2, 0, 3).reshape(2, PROMPTS, SEQ, HD)
    v = pieces[:, :, width_q + width_kv :].transpose(1, 0, 2).reshape(2, PROMPTS, SEQ, HD)

    early_here = (patch_mask * (patch_level[0] == 0)).astype(f32)
    early = [early_here] + [
        lax.ppermute(early_here, "patch", xor_pairs(n_p, j)) for j in range(1, kv_here)
    ]
    early = jnp.concatenate(early, axis=0)
    masks = jnp.broadcast_to(early[:, :, None], (kv_here, SEQ, HD))
    attended = attend(q, k, v, masks)

    mine = [attended[0]] + [
        lax.ppermute(attended[j], "patch", xor_pairs(n_p, j)) for j in range(1, kv_here)
    ]

    rows_dev = unembed.shape[0]
    local = scored_ids - lax.axis_index(("patch", "tp")) * rows_dev
    owned = (local >= 0) & (local < rows_dev)
    picked = jnp.where(
        owned[:, None], jnp.take(unembed, jnp.clip(local, 0, rows_dev - 1), axis=0), 0
    ).astype(bf16)
    scored = picked.shape[0]
    block = reduce_patch(picked.reshape(scored, n_p, n_t * sub).transpose(1, 0, 2))
    by_sub = block.reshape(scored, n_t, sub).transpose(1, 0, 2)
    if fused:
        score = lax.dynamic_index_in_dim(by_sub, me_t, 0, keepdims=False) + swap_tp(
            lax.dynamic_index_in_dim(by_sub, 1 - me_t, 0, keepdims=False)
        )
    else:
        score = sum(exchange_tp(by_sub))
    score = lax.all_gather(score, "patch", axis=0, tiled=True).reshape(n_p, scored, sub)

    row_mask = jnp.tile(patch_mask[0], PROMPTS) == 1
    share = tokens // n_t
    final_own = lax.dynamic_index_in_dim(
        final_full.reshape(n_p, n_t, sub), me_t, 1, keepdims=False
    ).reshape(1, n_p * sub)

    late_f = late_rows_here.astype(f32)
    late_final = (late_f * final_own).astype(bf16).reshape(rows_here, n_p, sub)
    late_logits = jnp.einsum("rpj,psj->rs", late_final, score, preferred_element_type=f32)
    late_squares = jnp.broadcast_to(
        jnp.sum(late_f * late_f, axis=1, keepdims=True), (rows_here, HD)
    )
    packed = jnp.concatenate([late_logits, late_squares], axis=1)
    packed = packed + swap_tp(packed) if n_t == 2 else lax.psum(packed, "tp")
    packed = gather_patch(packed).reshape(tokens, scored + HD)
    packed = lax.dynamic_slice_in_dim(packed, me_t * share, share, 0)
    late_total, late_sum = packed[:, :scored], packed[:, scored]
    is_late = row_mask & (patch_level[0] == 1)
    is_late = lax.dynamic_slice_in_dim(is_late, me_t * share, share, 0)

    def scored_shift(total, square_sum):
        total = jnp.where(is_late[:, None], late_total, total)
        scaling = lax.rsqrt(jnp.where(is_late, late_sum, square_sum) / D + EPSILON)
        return (total * scaling[:, None] - base_logits)[None]

    if fused:
        heads = mine + [swap_tp(x) for x in mine]
        code = jnp.where(row_mask, 1 + patch_level[0], 0)
        code = jnp.broadcast_to(code[:, None], (tokens, sub))
        place = jnp.stack([me_t, me_b]).astype(jnp.int32)
        base = splice(place, corrupt_full, clean_full, code, n_p * sub)
        parts = finish(place, heads, out_cols, base, final_own, score)
        logits, squares = (x.reshape(n_t, share, -1) for x in parts)

        def halves(x):
            return (
                lax.dynamic_index_in_dim(x, me_t, 0, keepdims=False),
                lax.dynamic_index_in_dim(x, 1 - me_t, 0, keepdims=False),
            )

        logits_keep, logits_send = halves(logits)
        squares_keep, squares_send = halves(squares[:, :, 0])
        square_sum = squares_keep + swap_tp(squares_send)
        total = logits_keep + swap_tp(logits_send.astype(bf16)).astype(f32)
        return scored_shift(total, square_sum)

    def in_order(slots):
        stacked = jnp.stack(slots)
        return jnp.concatenate(
            [
                lax.dynamic_index_in_dim(stacked, me_b ^ j, 0, keepdims=False)
                for j in range(kv_here)
            ],
            axis=1,
        )

    by_slot = [over_tp(x) for x in mine]
    rows_t = w_out.shape[0]
    early_rows = jnp.tile(early_here[0], PROMPTS)[:, None] > 0.5

    def own_features(x):
        own = lax.dynamic_index_in_dim(x.reshape(tokens, n_p, n_t, sub), me_t, 2, keepdims=False)
        return own.reshape(tokens, n_p * sub)

    residual = jnp.where(early_rows, own_features(clean_full), own_features(corrupt_full))
    residual = residual.astype(f32)
    for i in range(n_t):
        term = jnp.dot(
            in_order([slot[i] for slot in by_slot]),
            out_cols[i * rows_t : (i + 1) * rows_t],
            preferred_element_type=f32,
        )
        residual = residual + term.astype(bf16).astype(f32)
    squares = jnp.sum(residual * residual, axis=1)
    final_block = (residual * final_own).astype(bf16).reshape(tokens, n_p, sub)
    logits = jnp.einsum("rpj,psj->rs", final_block, score, preferred_element_type=f32)
    total = sum(exchange_tp(logits.reshape(n_t, share, -1)))
    square_sum = sum(exchange_tp(squares.reshape(n_t, share)))
    return scored_shift(total, square_sum)


def solution(mesh):
    placed = (
        P(None, "tp"),
        P(None, "patch", "tp"),
        P("patch"),
        P("patch", None),
        P("tp"),
        P("tp"),
        P("patch", "tp"),
        P("patch", "tp"),
        P("patch", "tp"),
        P("tp", "patch"),
        P(("patch", "tp"), None),
        P(),
        P("tp", None),
    )
    return jax.shard_map(
        on_device, mesh=mesh, in_specs=placed, out_specs=P("patch", "tp", None), check_vma=False
    )
```
